32 devices in a mesh: dp: 8 (over z, y), mp: 4 (over x, core).
Axes of the slice: x: 2, y: 2, z: 4, core: 2. Of those that a mesh axis runs over, the one named last changes fastest.
Arguments:
- tokens: bfloat16 [8, 1024, 1280], P('dp', 'mp'), may hold values from -6 to 6
- sizes: float32 [8, 1024], P('dp'), may hold values from 1 to 8
- ln1_gain: float32 [1280], replicated, may hold values from 0.25 to 1.75
- qkv_weight: bfloat16 [3, 1280, 1280], P(None, 'dp', 'mp'), may hold values from -0.15625 to 0.15625
- proj_weight: bfloat16 [1280, 1280], P('mp', 'dp'), may hold values from -0.15625 to 0.15625
- ln2_gain: float32 [1280], replicated, may hold values from 0.25 to 1.75
- fc1_weight: bfloat16 [1280, 5120], P('dp', 'mp'), may hold values from -0.15625 to 0.15625
- fc1_bias: float32 [5120], P('mp'), may hold values from -3 to 3
- fc2_weight: bfloat16 [5120, 1280], P('mp', 'dp'), may hold values from -0.078125 to 0.078125
- pair_source: int32 [8, 16], P('dp'), may hold values from 0 to 1022, as said below
- pair_target: int32 [8, 16], P('dp'), may hold values from 1 to 1023, as said below
- kept_order: int32 [8, 1008], P('dp'), may hold values from 0 to 1023, as said below
Outputs:
- merged_out: bfloat16 [8, 1008, 1280], P('dp', 'mp')
The draws below stay inside these ranges and needn't reach their ends.
Inputs may be any that keep to these rules, and one draw needn't show every extreme that they name: `pair_source`: in each image the 16 entries are distinct even token indices. `pair_target`: odd token indices; several sources may join the same target. `kept_order`: in each image every token index that is not in pair_source appears exactly once.
All inputs are finite; a program needn't handle non-finite values.
Results may differ from the reference program's by a relative error of at most 0.017.
Values may be sent and summed in bfloat16 or wider, within the bound.
A program may use at most 64 MiB of HBM per device.

```python
import math
import jax
import jax.numpy as jnp
from jax import lax

D = 1280
HEADS = 16
FF = 5120
N = 1024
R = 16
IMAGES = 8


def merge_plan(key):
    image_keys = jax.random.split(jax.random.fold_in(key, 7), IMAGES)

    def one_plan(image_key):
        first, second, third = jax.random.split(image_key, 3)
        shuffled = jax.random.permutation(first, N // 2).astype(jnp.int32)
        sources = 2 * shuffled[:R]
        targets = 2 * jax.random.randint(second, (R,), 0, N // 2).astype(jnp.int32) + 1
        kept_even = 2 * shuffled[R:]
        odd_tokens = 2 * jnp.arange(N // 2, dtype=jnp.int32) + 1
        remaining = jnp.concatenate([kept_even, odd_tokens])
        ordered = jax.random.permutation(third, remaining).astype(jnp.int32)
        return (sources, targets, ordered)
    return jax.vmap(one_plan)(image_keys)


def draw_pair_source(key, part):
    return merge_plan(key)[0]


def draw_pair_target(key, part):
    return merge_plan(key)[1]


def draw_kept_order(key, part):
    return merge_plan(key)[2]


def shard_levels(own_key, shape, cuts, low, high):
    def one(dim, blocks):
        heights = jax.random.uniform(jax.random.fold_in(jax.random.fold_in(own_key, 6), dim), (blocks,), jnp.float32, low / len(cuts), high / len(cuts))
        return jnp.repeat(jnp.exp(heights), shape[dim] // blocks).reshape((-1,) + (1,) * (len(shape) - dim - 1))

    factor_of = one(*cuts[0])
    for cut in cuts[1:]:
        factor_of = factor_of * one(*cut)
    return factor_of


def centred(key, extent, deviation, most, cuts=(), kind=jnp.bfloat16):
    values = deviation * jax.random.normal(key, extent, jnp.float32)
    if cuts:
        values = values * shard_levels(key, extent, cuts, -0.22, 0.18)
    return jnp.clip(values, -most, most).astype(kind)


def setup_inputs(seed: int = 0) -> dict:
    streams_of = jax.random.split(jax.random.key(seed), 13)
    return {
        "tokens": centred(streams_of[0], (IMAGES, N, D), 1.0, 6.0, ((0, 8), (1, 4))),
        "sizes": jnp.clip(jnp.exp(math.log(8.0) - 2.0794415 * jax.random.uniform(streams_of[1], (IMAGES, N), jnp.float32) ** shard_levels(streams_of[1], (IMAGES, N), ((0, 8),), -0.2, 0.2)), 1.0, 8.0),
        "ln1_gain": jnp.clip(1.0 + 0.15 * jax.random.normal(streams_of[2], (D,), jnp.float32), 0.25, 1.75),
        "qkv_weight": centred(streams_of[3], (3, D, D), D ** -0.5, 0.15625, ((1, 8), (2, 4))),
        "proj_weight": centred(streams_of[4], (D, D), D ** -0.5, 0.15625, ((0, 4), (1, 8))),
        "ln2_gain": jnp.clip(1.0 + 0.15 * jax.random.normal(streams_of[5], (D,), jnp.float32), 0.25, 1.75),
        "fc1_weight": centred(streams_of[6], (D, FF), D ** -0.5, 0.15625, ((0, 8), (1, 4))),
        "fc1_bias": centred(streams_of[7], (FF,), 0.5, 3.0, ((0, 4),), jnp.float32),
        "fc2_weight": centred(streams_of[8], (FF, D), FF ** -0.5, 0.078125, ((0, 4), (1, 8))),
        "pair_source": draw_pair_source(jax.random.fold_in(streams_of[12], 71), 0),
        "pair_target": draw_pair_target(jax.random.fold_in(streams_of[12], 71), 0),
        "kept_order": draw_kept_order(jax.random.fold_in(streams_of[12], 71), 0),
    }


def layer_norm(values, gain):
    center = values - lax.optimization_barrier(jnp.mean(values, axis=-1, keepdims=True))
    spread = lax.optimization_barrier(jnp.mean(center * center, axis=-1, keepdims=True))
    return center * lax.rsqrt(spread + 1e-06) * gain

def one_image(tokens, sizes, source_ids, target_ids, order, ln1_gain, qkv_weight, proj_weight, ln2_gain, fc1_weight, fc1_bias, fc2_weight):
    width = tokens.shape[1]
    head_size = width // HEADS
    base = tokens.astype(jnp.float32)
    normed = layer_norm(base, ln1_gain).astype(jnp.bfloat16)
    query = jnp.dot(normed, qkv_weight[0], preferred_element_type=jnp.float32).astype(jnp.bfloat16)
    keys = jnp.dot(normed, qkv_weight[1], preferred_element_type=jnp.float32).astype(jnp.bfloat16)
    values = jnp.dot(normed, qkv_weight[2], preferred_element_type=jnp.float32).astype(jnp.bfloat16)
    length = tokens.shape[0]
    query = query.reshape(length, HEADS, head_size).astype(jnp.float32)
    keys = keys.reshape(length, HEADS, head_size).astype(jnp.float32)
    values = values.reshape(length, HEADS, head_size).astype(jnp.float32)
    scores = jnp.einsum('qhe,khe->hqk', query, keys) / math.sqrt(head_size) + jnp.log(sizes)[None, None, :]
    weights = jax.nn.softmax(scores, axis=-1).astype(jnp.bfloat16)
    attended = jnp.einsum('hqk,khe->qhe', weights.astype(jnp.float32), values).astype(jnp.bfloat16)
    attended = attended.reshape(length, width)
    residual = base + jnp.dot(attended, proj_weight, preferred_element_type=jnp.float32)
    positions = jnp.arange(length, dtype=jnp.int32)
    hits = (positions[None, :] == source_ids[:, None]).astype(jnp.int32)
    destination = positions + lax.optimization_barrier(jnp.sum(hits * (target_ids[:, None] - positions[None, :]), axis=0))
    table = (order[:, None] == destination[None, :]).astype(jnp.float32)
    numerator = jnp.dot(table, sizes[:, None] * residual, precision=lax.Precision.HIGHEST)
    merged_size = jnp.dot(table, sizes, precision=lax.Precision.HIGHEST)
    merged = numerator / merged_size[:, None]
    normed_two = layer_norm(merged, ln2_gain).astype(jnp.bfloat16)
    hidden = jax.nn.gelu(jnp.dot(normed_two, fc1_weight, preferred_element_type=jnp.float32) + fc1_bias).astype(jnp.bfloat16)
    return (merged + jnp.dot(hidden, fc2_weight, preferred_element_type=jnp.float32)).astype(jnp.bfloat16)

def reference(tokens, sizes, ln1_gain, qkv_weight, proj_weight, ln2_gain, fc1_weight, fc1_bias, fc2_weight, pair_source, pair_target, kept_order):

    def apply(item):
        return one_image(item[0], item[1], item[2], item[3], item[4], ln1_gain, qkv_weight, proj_weight, ln2_gain, fc1_weight, fc1_bias, fc2_weight)
    return lax.map(apply, (tokens, sizes, pair_source, pair_target, kept_order))
```

```python
import functools
import math

import jax
import jax.numpy as jnp
from jax import lax
from jax.experimental import pallas as pl
from jax.experimental.pallas import tpu as pltpu
from jax.sharding import PartitionSpec as P

HEADS = 16


def layer_norm(values, gain):
    center = values - jnp.mean(values, axis=-1, keepdims=True)
    spread = jnp.mean(center * center, axis=-1, keepdims=True)
    return center * lax.rsqrt(spread + 1e-06) * gain


def powers(count):
    bits = []
    bit = 1
    while bit < count:
        bits.append(bit)
        bit *= 2
    return bits


def toggled(index, mask):
    for bit in powers(mask + 1):
        if mask & bit:
            index = index + bit * (1 - 2 * lax.rem(lax.div(index, bit), 2))
    return index


def greet(peers):
    barrier = pltpu.get_barrier_semaphore()
    for axis, peer in peers:
        pl.semaphore_signal(
            barrier, inc=1, device_id={axis: peer}, device_id_type=pl.DeviceIdType.MESH
        )
    pl.semaphore_wait(barrier, len(peers))


class Copies:
    def __init__(self, send, recv):
        self.send, self.recv, self.made = send, recv, []

    def start(self, source, target, axis, peer):
        number = len(self.made)
        copy = pltpu.make_async_remote_copy(
            src_ref=source,
            dst_ref=target,
            send_sem=self.send.at[number],
            recv_sem=self.recv.at[number],
            device_id={axis: peer},
            device_id_type=pl.DeviceIdType.MESH,
        )
        copy.start()
        self.made.append(copy)
        return copy


def rows_of(out, owner, rows):
    span = pl.ds(pl.multiple_of(owner * rows, 16), rows)
    if len(out.shape) == 3:
        return out.at[:, span, :]
    return out.at[span, :]


class Waits:
    def __init__(self):
        self.seen = set()

    def ready(self, copy):
        if id(copy) not in self.seen:
            copy.wait_recv()
            self.seen.add(id(copy))


def dp_peers(dp):
    me = lax.axis_index("dp")
    return me, toggled(me, 1), lax.rem(me + 2, dp), lax.rem(me + dp - 2, dp)


def start_dp(own, out, copies, dp):
    me, pair, after, before = dp_peers(dp)
    here = rows_of(out, me, own.shape[-2])
    return [copies.start(own, here, "dp", peer) for peer in (pair, after, before)]


def relay_dp(own, out, copies, waits, state, dp, step):
    me, pair, after, before = dp_peers(dp)
    ring = dp // 2
    rows = own.shape[-2]
    other, forward, backward = state
    block = rows_of(out, lax.rem(me - 2 * step + 2 * dp, dp), rows)
    waits.ready(forward)
    if step < ring // 2:
        state[1] = copies.start(block, block, "dp", after)
    copies.start(block, block, "dp", pair)
    if step < ring - step:
        block = rows_of(out, toggled(lax.rem(me + 2 * (step - 1), dp), 1), rows)
        waits.ready(other)
        state[0] = copies.start(block, block, "dp", before)
        if step + 1 < ring - step - 1:
            block = rows_of(out, lax.rem(me + 2 * step, dp), rows)
            waits.ready(backward)
            state[2] = copies.start(block, block, "dp", before)


def gather_kernel(dp, mp, *refs):
    own, out = refs[:2], refs[2:4]
    send, recv, local = refs[4:]
    at = lax.axis_index("mp")
    me, pair, after, before = dp_peers(dp)
    greet(
        [("mp", toggled(at, bit)) for bit in powers(mp)]
        + [("dp", pair), ("dp", after), ("dp", before)]
    )
    copies, waits = Copies(send, recv), Waits()
    heads = start_dp(own[1], out[1], copies, dp)
    mine = rows_of(out[0], at, own[0].shape[0])
    bits = list(reversed(powers(mp)))
    here = {bit: copies.start(own[0], mine, "mp", toggled(at, bit)) for bit in bits}
    stays = []
    for number, owner in ((0, at), (1, me)):
        keep = pltpu.make_async_copy(
            own[number], rows_of(out[number], owner, own[number].shape[-2]), local.at[number]
        )
        keep.start()
        stays.append(keep)
    relay_dp(own[1], out[1], copies, waits, heads, dp, 1)
    held = [0]
    for bit in bits:
        for k in list(held):
            if k:
                waits.ready(here[k])
                block = rows_of(out[0], toggled(at, k), own[0].shape[0])
                here[k ^ bit] = copies.start(block, block, "mp", toggled(at, bit))
            held.append(k ^ bit)
    for step in range(2, dp // 4 + 1):
        relay_dp(own[1], out[1], copies, waits, heads, dp, step)
    for copy in copies.made:
        waits.ready(copy)
        copy.wait_send()
    for keep in stays:
        keep.wait()


def gather_all(normed, heads):
    dp, mp = lax.axis_size("dp"), lax.axis_size("mp")
    total = (mp - 1) + (dp - 1)
    shapes = [
        (mp * normed.shape[0], normed.shape[1]),
        (dp * heads.shape[0], heads.shape[1]),
    ]
    return pl.pallas_call(
        functools.partial(gather_kernel, dp, mp),
        out_shape=[jax.ShapeDtypeStruct(shape, jnp.bfloat16) for shape in shapes],
        in_specs=[pl.BlockSpec(memory_space=pltpu.VMEM)] * 2,
        out_specs=[pl.BlockSpec(memory_space=pl.ANY)] * 2,
        scratch_shapes=[
            pltpu.SemaphoreType.DMA((total,)),
            pltpu.SemaphoreType.DMA((total,)),
            pltpu.SemaphoreType.DMA((2,)),
        ],
        compiler_params=pltpu.CompilerParams(collective_id=0, has_side_effects=True),
        cost_estimate=pl.CostEstimate(
            flops=10**10, bytes_accessed=10**8, transcendentals=0
        ),
        name="gather_all",
    )(normed, heads)


def reduce_kernel(dp, mp, last, *refs):
    if last:
        parts, extra, out, held, landing, send, recv = refs
    else:
        parts, extra, own, out, whole, weight, held, landing, normed, send, recv, local = refs
    at = lax.axis_index("mp")
    peers = [("mp", toggled(at, bit)) for bit in powers(mp)]
    if not last:
        peers += [("dp", peer) for peer in dp_peers(dp)[1:]]
    greet(peers)
    copies, waits = Copies(send, recv), Waits()
    slots = 0
    stored = {k: None for k in range(mp)}
    if not last:
        state = start_dp(own, weight, copies, dp)
        rest = pltpu.make_async_copy(
            own, rows_of(weight, lax.axis_index("dp"), own.shape[0]), local.at[1]
        )
        rest.start()

    def source(k):
        return parts.at[toggled(at, k)] if stored[k] is None else held.at[k]

    for bit in powers(mp):
        moving = [k for k in reversed(range(mp)) if k in stored and k & bit]
        flights = []
        for k in moving:
            flights.append(
                (k, slots, copies.start(source(k), landing.at[slots], "mp", toggled(at, bit)))
            )
            slots += 1
        for k, slot, copy in flights:
            waits.ready(copy)
            kept = k ^ bit
            total = source(kept)[...].astype(jnp.float32) + landing[slot].astype(jnp.float32)
            if 2 * bit < mp:
                held[kept] = total.astype(jnp.bfloat16)
                stored[kept] = True
            del stored[k]
        if not last and bit == 1:
            relay_dp(own, weight, copies, waits, state, dp, 1)
    if last:
        out[...] = (extra[...] + total).astype(out.dtype)
    else:
        out[...] = total
        normed[...] = layer_norm(total, extra[...]).astype(jnp.bfloat16)
        keep = pltpu.make_async_copy(normed, whole.at[at], local.at[0])
        keep.start()
        bits = list(reversed(powers(mp)))
        here = {
            bit: copies.start(normed, whole.at[at], "mp", toggled(at, bit)) for bit in bits
        }
        for step in range(2, dp // 4 + 1):
            relay_dp(own, weight, copies, waits, state, dp, step)
        near = [0]
        for bit in bits:
            for k in list(near):
                if k:
                    waits.ready(here[k])
                    block = whole.at[toggled(at, k)]
                    here[k ^ bit] = copies.start(block, block, "mp", toggled(at, bit))
                near.append(k ^ bit)
        keep.wait()
        rest.wait()
    for copy in copies.made:
        waits.ready(copy)
        copy.wait_send()


def reduce_parts(parts, extra, own=None):
    mp, rows, width = parts.shape
    dp = lax.axis_size("dp")
    last = own is None
    operands = [parts, extra] if last else [parts, extra, own]
    vmem = pl.BlockSpec(memory_space=pltpu.VMEM)
    out_shape = [
        jax.ShapeDtypeStruct((rows, width), jnp.bfloat16 if last else jnp.float32)
    ]
    out_specs = [vmem]
    scratch = [
        pltpu.VMEM((mp, rows, width), jnp.bfloat16),
        pltpu.VMEM((mp - 1, rows, width), jnp.bfloat16),
    ]
    total = mp - 1
    if not last:
        out_shape.append(jax.ShapeDtypeStruct((mp, rows, width), jnp.bfloat16))
        out_shape.append(jax.ShapeDtypeStruct((dp * own.shape[0], own.shape[1]), jnp.bfloat16))
        out_specs += [pl.BlockSpec(memory_space=pl.ANY)] * 2
        scratch.append(pltpu.VMEM((rows, width), jnp.bfloat16))
        total = 2 * total + dp - 1
    scratch += [pltpu.SemaphoreType.DMA((total,)), pltpu.SemaphoreType.DMA((total,))]
    if not last:
        scratch.append(pltpu.SemaphoreType.DMA((2,)))
    return pl.pallas_call(
        functools.partial(reduce_kernel, dp, mp, last),
        out_shape=out_shape,
        in_specs=[vmem] * len(operands),
        out_specs=out_specs,
        scratch_shapes=scratch,
        compiler_params=pltpu.CompilerParams(
            collective_id=2 if last else 1, has_side_effects=True
        ),
        cost_estimate=pl.CostEstimate(
            flops=10**10, bytes_accessed=10**8, transcendentals=0
        ),
        name="reduce_last" if last else "reduce_norm_gather",
    )(*operands)


def shards(
    tokens,
    sizes,
    ln1_gain,
    qkv_weight,
    proj_weight,
    ln2_gain,
    fc1_weight,
    fc1_bias,
    fc2_weight,
    pair_source,
    pair_target,
    kept_order,
):
    images, own_tokens, width = tokens.shape
    length = sizes.shape[1]
    kept_total = kept_order.shape[1]
    count = lax.axis_size("mp")
    me = lax.axis_index("mp")
    kept_own = kept_total // count
    padded = -(-kept_own // 16) * 16
    head_size = width // HEADS
    local_width = qkv_weight.shape[2]
    local_heads = local_width // head_size

    base = tokens.astype(jnp.float32)
    normed = layer_norm(base, ln1_gain).astype(jnp.bfloat16)
    whole, heads_whole = gather_all(
        normed.reshape(own_tokens, width),
        jnp.concatenate(
            [qkv_weight[0], qkv_weight[1], qkv_weight[2], proj_weight.T], axis=1
        ),
    )
    whole = whole[None]
    whole, heads_whole, late = lax.optimization_barrier((whole, heads_whole, fc1_weight))
    fc1 = lax.all_gather(late, "dp", axis=0, tiled=True)

    positions = jnp.arange(length, dtype=jnp.int32)
    order = jnp.pad(
        kept_order.reshape(images, count, kept_own),
        ((0, 0), (0, 0), (0, padded - kept_own)),
        constant_values=-1,
    ).reshape(images, count * padded)
    hits = positions[None, None, :] == pair_source[:, :, None]
    destination = positions[None, :] + jnp.sum(
        jnp.where(hits, pair_target[:, :, None] - positions[None, None, :], 0), axis=1
    )
    joins = order[:, :, None] == destination[:, None, :]
    shares = jnp.where(joins, sizes[:, None, :], 0.0)
    merged_size = jnp.sum(shares, axis=2, keepdims=True)
    shares = (shares / jnp.where(merged_size > 0, merged_size, 1.0)).astype(jnp.bfloat16)
    own_shares = lax.dynamic_slice_in_dim(shares, me * own_tokens, own_tokens, 2)

    projected = jnp.einsum(
        "ind,df->inf", whole, heads_whole[:, : 3 * local_width], preferred_element_type=jnp.float32
    ).astype(jnp.bfloat16)
    shaped = [
        projected[:, :, c * local_width : (c + 1) * local_width].reshape(
            images, length, local_heads, head_size
        )
        for c in range(3)
    ]
    size_bias = jnp.log(sizes)[:, None, None, :]
    block = min(512, length)
    outputs = []
    for begin in range(0, length, block):
        scores = (
            jnp.einsum(
                "iqhe,ikhe->ihqk",
                shaped[0][:, begin : begin + block],
                shaped[1],
                preferred_element_type=jnp.float32,
            )
            / math.sqrt(head_size)
            + size_bias
        )
        weights = jax.nn.softmax(scores, axis=-1).astype(jnp.bfloat16)
        outputs.append(
            jnp.einsum("ihqk,ikhe->iqhe", weights, shaped[2], preferred_element_type=jnp.float32)
            .astype(jnp.bfloat16)
            .reshape(images, block, local_width)
        )
    attended = jnp.concatenate(outputs, axis=1)

    joined = jnp.einsum(
        "ijn,ind->ijd", shares, attended, preferred_element_type=jnp.float32
    ).astype(jnp.bfloat16)

    left, right = lax.optimization_barrier(
        (
            jnp.concatenate([joined, own_shares], axis=2),
            jnp.concatenate([heads_whole[:, 3 * local_width :].T, tokens[0]], axis=0),
        )
    )
    parts = jnp.einsum("ijd,de->ije", left, right, preferred_element_type=jnp.float32)
    parts = parts.astype(jnp.bfloat16).reshape(count, padded, width)
    merged, gathered, fc2 = reduce_parts(parts, ln2_gain.reshape(1, width), fc2_weight.T)
    hidden_sum = jnp.einsum(
        "md,df->mf", gathered.reshape(count * padded, width), fc1,
        preferred_element_type=jnp.float32,
    )
    hidden = jax.nn.gelu(hidden_sum + fc1_bias).astype(jnp.bfloat16)
    partial_out = jnp.einsum("mf,df->md", hidden, fc2, preferred_element_type=jnp.float32)
    partial_out = partial_out.astype(jnp.bfloat16).reshape(count, padded, width)
    out = reduce_parts(partial_out, merged)[0]
    return out[None, :kept_own]


def solution(mesh):
    return jax.shard_map(
        shards,
        mesh=mesh,
        in_specs=(
            P("dp", "mp", None),
            P("dp", None),
            P(),
            P(None, "dp", "mp"),
            P("mp", "dp"),
            P(),
            P("dp", "mp"),
            P("mp"),
            P("mp", "dp"),
            P("dp", None),
            P("dp", None),
            P("dp", None),
        ),
        out_specs=P("dp", "mp", None),
        check_vma=False,
    )
```
